128 devices in a mesh: row: 8 (over z, core), col: 16 (over y, x).
Axes of the slice: x: 4, y: 4, z: 4, core: 2. Of those that a mesh axis runs over, the one named last changes fastest.
Arguments:
- item_table: float32 [5242880, 128], P(('row', 'col')), may hold values from -6 to 6
- owner_ids: int32 [16384, 50], P(('row', 'col')), may hold values from 0 to 127, as said below
- row_ids: int32 [16384, 50], P(('row', 'col')), may hold values from 0 to 40959
- lengths: int32 [16384], P(('row', 'col')), may hold values from 25 to 50
- dense_input: bfloat16 [16384, 256], P(('row', 'col')), may hold values from -6 to 6
- w_bottom: bfloat16 [256, 256], replicated, may hold values from -0.375 to 0.375
Outputs:
- features: float32 [16384, 384], P(('row', 'col'))
The draws below stay inside these ranges and needn't reach their ends.
Inputs may be any that keep to these rules, and one draw needn't show every extreme that they name: Among the live positions (p < lengths[u]) of the 128 users of one device, at most 75 have the same owner_ids value; in every draw some owner_ids values receive exactly 75 live positions from every device.
All inputs are finite; a program needn't handle non-finite values.
Results may differ from the reference program's by a relative error of at most 0.0003.
Values sent between devices are 32-bit elements; how exact they have to be, the bound alone decides.
No kernel may reach another device: no remote copies, remote signals or barrier semaphores. Data moves between devices by JAX's collectives and lax.ppermute only.
A program may use at most 128 MiB of HBM per device.

```python
import jax
import jax.numpy as jnp
from jax import lax

DIM = 128
DENSE = 256
HIST = 50
ROWS_DEV = 40960
U_DEV = 128
OWNERS = 128
USERS = 16384
ITEMS = 5242880
CAP = 75
HOT = 8


def history_plan(key):
    seed_key = jax.random.fold_in(key, 7103)
    hot_owners = jax.random.permutation(jax.random.fold_in(seed_key, 1), OWNERS)[:HOT]
    hot_flag = jnp.zeros((OWNERS,), jnp.int32).at[hot_owners].set(1)
    hot_rows = jax.random.randint(jax.random.fold_in(seed_key, 2), (OWNERS, 16), 0, ROWS_DEV)
    slot_total = OWNERS * CAP
    pos_count = U_DEV * HIST

    def one_source(source):
        source_key = jax.random.fold_in(seed_key, 100 + source)
        lengths_dev = jax.random.randint(jax.random.fold_in(source_key, 1), (U_DEV,), HIST // 2, HIST + 1)
        position = lax.broadcasted_iota(jnp.int32, (U_DEV, HIST), 1)
        live_flag = (position < lengths_dev[:, None]).reshape(-1).astype(jnp.int32)
        slot_owner = jnp.arange(slot_total, dtype=jnp.int32) // CAP
        noise_part = jax.random.randint(jax.random.fold_in(source_key, 2), (slot_total,), 0, 1024)
        tiebreak = jax.random.permutation(jax.random.fold_in(source_key, 3), slot_total).astype(jnp.int32)
        slot_score = (noise_part + 2048 * hot_flag[slot_owner]) * slot_total + tiebreak
        chosen = lax.top_k(slot_score, pos_count)[1].astype(jnp.int32)
        live_first = (1 - live_flag) * pos_count + jax.random.permutation(jax.random.fold_in(source_key, 4), pos_count).astype(jnp.int32)
        ranked = jnp.argsort(live_first)
        owners_out = jnp.zeros((pos_count,), jnp.int32).at[ranked].set(chosen // CAP)
        hot_choice = jax.random.randint(jax.random.fold_in(source_key, 5), (pos_count,), 0, 16)
        hot_coin = jax.random.randint(jax.random.fold_in(source_key, 6), (pos_count,), 0, 4)
        uniform_row = jax.random.randint(jax.random.fold_in(source_key, 7), (pos_count,), 0, ROWS_DEV)
        rows_out = jnp.where(hot_coin == 0, hot_rows[owners_out, hot_choice], uniform_row)
        return (owners_out, rows_out.astype(jnp.int32), lengths_dev.astype(jnp.int32))
    return jax.vmap(one_source)(jnp.arange(OWNERS, dtype=jnp.int32))


def draw_owner_ids(key, part):
    owners_out, rows_out, lengths_all = history_plan(key)
    return owners_out.reshape(USERS, HIST)


def draw_row_ids(key, part):
    owners_out, rows_out, lengths_all = history_plan(key)
    return rows_out.reshape(USERS, HIST)


def draw_lengths(key, part):
    owners_out, rows_out, lengths_all = history_plan(key)
    return lengths_all.reshape(USERS)


def level_of(key, shape, pieces, least, top_value):
    loudness = 1.0
    for axis_at, blocks in pieces:
        steps = jax.random.uniform(jax.random.fold_in(jax.random.fold_in(key, 6), axis_at), (blocks,), jnp.float32, least / len(pieces), top_value / len(pieces))
        loudness = loudness * jnp.repeat(jnp.exp(steps), shape[axis_at] // blocks).reshape((-1,) + (1,) * (len(shape) - 1 - axis_at))
    return loudness


def scatter_about(stream_key, shape, width, bound, pieces=(), kind=jnp.bfloat16):
    entries = jax.random.normal(stream_key, shape, jnp.float32) * width
    if len(pieces) > 0:
        entries = level_of(stream_key, shape, pieces, -0.22, 0.18) * entries
    return jnp.clip(entries, min=-bound, max=bound).astype(kind)


def setup_inputs(seed: int = 0) -> dict:
    splits = jax.random.split(jax.random.key(seed), 7)
    return {
        "item_table": scatter_about(splits[0], (ITEMS, DIM), 1.0, 6.0, ((0, 128),), jnp.float32),
        "owner_ids": draw_owner_ids(jax.random.fold_in(splits[6], 71), 0),
        "row_ids": draw_row_ids(jax.random.fold_in(splits[6], 71), 0),
        "lengths": draw_lengths(jax.random.fold_in(splits[6], 71), 0),
        "dense_input": scatter_about(splits[4], (USERS, DENSE), 1.0, 6.0, ((0, 128),)),
        "w_bottom": scatter_about(splits[5], (DENSE, DENSE), DENSE ** -0.5, 0.375),
    }


def reference(item_table, owner_ids, row_ids, lengths, dense_input, w_bottom):
    item_index = (owner_ids * ROWS_DEV + row_ids).astype(jnp.int32)
    position = lax.broadcasted_iota(jnp.int32, owner_ids.shape, 1)
    live_mask = (position < lengths[:, None]).astype(item_table.dtype)
    index_blocks = item_index.reshape(USERS // U_DEV, U_DEV, HIST)
    mask_blocks = live_mask.reshape(USERS // U_DEV, U_DEV, HIST)

    def pool_block(bundle):
        index_block, mask_block = bundle
        gathered = jnp.take(item_table, index_block.reshape(-1), axis=0).reshape(U_DEV, HIST, DIM)
        return jnp.sum(gathered * mask_block[:, :, None], axis=1)

    totals = lax.map(pool_block, (index_blocks, mask_blocks)).reshape(USERS, DIM)
    pooled = totals / lengths[:, None].astype(jnp.float32)
    hidden = jnp.dot(dense_input, w_bottom, preferred_element_type=jnp.float32)
    return jnp.concatenate([pooled, jax.nn.silu(hidden)], axis=1)
```

```python
import functools

import jax
import jax.numpy as jnp
from jax import lax
from jax.experimental import pallas as pl
from jax.experimental.pallas import tpu as pltpu
from jax.sharding import PartitionSpec as P

SLOT_PAD = 80
LANES = 128
FIRST_SLOTS = 20


def round_up(value, unit):
    return (value + unit - 1) // unit * unit


def exchange(buffer):
    return lax.all_to_all(buffer, ("row", "col"), split_axis=0, concat_axis=0, tiled=True)


def route_kernel(me_ref, owner_ref, row_ref, len_ref, rows_out, users_out, assign_ref, value_ref):
    hist_len, user_count = owner_ref.shape
    owner_count = rows_out.shape[0]
    lens = len_ref[...]
    owner_iota = lax.broadcasted_iota(jnp.int32, (owner_count, user_count), 0)
    slot_iota = lax.broadcasted_iota(jnp.int32, (SLOT_PAD, user_count), 0)
    user_iota = lax.broadcasted_iota(jnp.int32, (1, user_count), 1)
    earlier = lax.broadcasted_iota(jnp.int32, (user_count, 2 * user_count), 0)
    later = lax.broadcasted_iota(jnp.int32, (user_count, 2 * user_count), 1)
    counter = jnp.where((earlier < later) | (later >= user_count), 1.0, 0.0).astype(jnp.bfloat16)
    offset = jnp.zeros((owner_count, user_count), jnp.float32)
    for h in range(hist_len):
        owners = jnp.where(h < lens, owner_ref[h : h + 1, :], -1)
        hits = owners == owner_iota
        assign = jnp.where(hits, 1.0, 0.0).astype(jnp.bfloat16)
        assign_ref[:, h * user_count : (h + 1) * user_count] = assign
        counts = jnp.dot(assign, counter, preferred_element_type=jnp.float32)
        ahead = counts[:, :user_count] + offset
        rank = jnp.sum(jnp.where(hits, ahead, 0.0), axis=0, keepdims=True).astype(jnp.int32)
        offset = offset + counts[:, user_count:]
        spot = rank == slot_iota
        rows = row_ref[h : h + 1, :]
        high = (rows >> 8).astype(jnp.float32)
        low = (rows & 255).astype(jnp.float32)
        name = (user_iota + 1).astype(jnp.float32)
        for part, content in enumerate((high, low, name)):
            value_ref[part * SLOT_PAD : (part + 1) * SLOT_PAD, h * user_count : (h + 1) * user_count] = (
                jnp.where(spot, content, 0.0).astype(jnp.bfloat16)
            )
    packed = lax.dot_general(
        assign_ref[...], value_ref[...], (((1,), (1,)), ((), ())), preferred_element_type=jnp.float32
    )
    names = packed[:, 2 * SLOT_PAD :]
    spare = me_ref[0, 0] * SLOT_PAD + lax.broadcasted_iota(jnp.int32, names.shape, 1)
    table_rows = (packed[:, :SLOT_PAD] * 256.0 + packed[:, SLOT_PAD : 2 * SLOT_PAD]).astype(jnp.int32)
    table_rows = jnp.where(names > 0.0, table_rows, spare)
    fill = jnp.zeros((owner_count, LANES - SLOT_PAD), jnp.int32)
    rows_out[...] = jnp.concatenate([table_rows, fill], axis=1)
    users_out[...] = jnp.concatenate([names.astype(jnp.int32), fill], axis=1)


def route(me, owner_t, row_t, lengths, owner_count):
    hist_len, user_count = owner_t.shape
    pos_count = hist_len * user_count
    shape = jax.ShapeDtypeStruct((owner_count, LANES), jnp.int32)
    return pl.pallas_call(
        route_kernel,
        in_specs=[
            pl.BlockSpec(memory_space=pltpu.SMEM),
            pl.BlockSpec(memory_space=pltpu.VMEM),
            pl.BlockSpec(memory_space=pltpu.VMEM),
            pl.BlockSpec(memory_space=pltpu.VMEM),
        ],
        out_shape=(shape, shape),
        scratch_shapes=[
            pltpu.VMEM((owner_count, pos_count), jnp.bfloat16),
            pltpu.VMEM((3 * SLOT_PAD, pos_count), jnp.bfloat16),
        ],
        name="route",
    )(jnp.full((1, 1), me, jnp.int32), owner_t, row_t, lengths.reshape(1, user_count))


def fetch_kernel(first, count, groups, wanted_ref, table_ref, out_ref, stage_ref, in_sems, out_sems):
    sources = wanted_ref.shape[0]
    per_group = sources // groups
    span = per_group * count

    def issue(group):
        def one_source(index, carry):
            source = group * per_group + index
            for c in range(count):
                pltpu.make_async_copy(
                    table_ref.at[pl.ds(wanted_ref[source, 0, first + c], 1), :],
                    stage_ref.at[pl.ds(source * count + c, 1), :],
                    in_sems.at[group],
                ).start(priority=c % 2)
            return carry

        lax.fori_loop(0, per_group, one_source, 0)

    def store(group):
        place = pl.ds(group * span, span)
        return pltpu.make_async_copy(stage_ref.at[place, :], out_ref.at[place, :], out_sems.at[group])

    def arrive(group):
        place = pl.ds(group * span, span)
        pltpu.make_async_copy(table_ref.at[pl.ds(0, span), :], stage_ref.at[place, :], in_sems.at[group]).wait()
        store(group).start()

    for group in range(groups):
        issue(group)
        if group > 0:
            arrive(group - 1)
    arrive(groups - 1)
    for group in range(groups):
        store(group).wait()


def fetch(wanted, item_table, first, count, groups):
    sources = wanted.shape[0]
    dim = item_table.shape[1]
    return pl.pallas_call(
        functools.partial(fetch_kernel, first, count, groups),
        in_specs=[pl.BlockSpec(memory_space=pltpu.SMEM), pl.BlockSpec(memory_space=pl.ANY)],
        out_specs=pl.BlockSpec(memory_space=pl.ANY),
        out_shape=jax.ShapeDtypeStruct((sources * count, dim), jnp.float32),
        scratch_shapes=[
            pltpu.VMEM((sources * count, dim), jnp.float32),
            pltpu.SemaphoreType.DMA((groups,)),
            pltpu.SemaphoreType.DMA((groups,)),
        ],
        cost_estimate=pl.CostEstimate(
            flops=sources * count * 4000, bytes_accessed=sources * count * dim * 8, transcendentals=0
        ),
        name="fetch",
    )(wanted, item_table)


def add_rows(slot_ref, rows_ref, acc_ref):
    user_count = acc_ref.shape[0]
    rows = rows_ref[...]
    high = rows.astype(jnp.bfloat16)
    low = (rows - high.astype(jnp.float32)).astype(jnp.bfloat16)
    users = lax.broadcasted_iota(jnp.int32, (user_count, rows.shape[0]), 0) + 1
    selector = jnp.where(slot_ref[...] == users, 1.0, 0.0).astype(jnp.bfloat16)
    acc_ref[...] += jnp.dot(
        selector, jnp.concatenate([high, low], axis=1), preferred_element_type=jnp.float32
    )


def pool_first_kernel(slot_ref, rows_ref, acc_ref):
    @pl.when(pl.program_id(0) == 0)
    def _():
        acc_ref[...] = jnp.zeros_like(acc_ref)

    add_rows(slot_ref, rows_ref, acc_ref)


def pool_last_kernel(slot_ref, rows_ref, start_ref, len_ref, dense_ref, out_ref, acc_ref):
    step = pl.program_id(0)
    dim = rows_ref.shape[1]

    @pl.when(step == 0)
    def _():
        acc_ref[...] = start_ref[...]

    add_rows(slot_ref, rows_ref, acc_ref)

    @pl.when(step == pl.num_programs(0) - 1)
    def _():
        total = acc_ref[:, :dim] + acc_ref[:, dim:]
        out_ref[:, :dim] = total / len_ref[...]
        out_ref[:, dim:] = dense_ref[...]


def pool_first(slots, rows, user_count, steps):
    count, dim = rows.shape
    chunk = count // steps
    return pl.pallas_call(
        pool_first_kernel,
        grid=(steps,),
        in_specs=[pl.BlockSpec((1, chunk), lambda i: (0, i)), pl.BlockSpec((chunk, dim), lambda i: (i, 0))],
        out_specs=pl.BlockSpec((user_count, 2 * dim), lambda i: (0, 0)),
        out_shape=jax.ShapeDtypeStruct((user_count, 2 * dim), jnp.float32),
        cost_estimate=pl.CostEstimate(flops=count * 4000, bytes_accessed=count * dim * 4, transcendentals=0),
        name="pool_first",
    )(slots, rows)


def pool_last(slots, rows, start, lens, dense_out, steps):
    count, dim = rows.shape
    user_count, dense_dim = dense_out.shape
    chunk = count // steps
    return pl.pallas_call(
        pool_last_kernel,
        grid=(steps,),
        in_specs=[
            pl.BlockSpec((1, chunk), lambda i: (0, i)),
            pl.BlockSpec((chunk, dim), lambda i: (i, 0)),
            pl.BlockSpec((user_count, 2 * dim), lambda i: (0, 0)),
            pl.BlockSpec((user_count, dim), lambda i: (0, 0)),
            pl.BlockSpec((user_count, dense_dim), lambda i: (0, 0)),
        ],
        out_specs=pl.BlockSpec((user_count, dim + dense_dim), lambda i: (0, 0)),
        out_shape=jax.ShapeDtypeStruct((user_count, dim + dense_dim), jnp.float32),
        scratch_shapes=[pltpu.VMEM((user_count, 2 * dim), jnp.float32)],
        name="pool_last",
    )(slots, rows, start, lens, dense_out)


def per_device(item_table, owner_ids, row_ids, lengths, dense_input, w_bottom):
    user_count, hist_len = owner_ids.shape
    dim = item_table.shape[1]
    owner_count = lax.axis_size("row") * lax.axis_size("col")
    capacity = 3 * user_count * hist_len // (2 * owner_count)
    ahead = FIRST_SLOTS
    behind = capacity - ahead
    me = lax.axis_index("row") * lax.axis_size("col") + lax.axis_index("col")
    table_rows, slot_users = route(me, owner_ids.T, row_ids.T, lengths, owner_count)
    wanted = exchange(table_rows.reshape(owner_count, 1, LANES))
    fetched_one = fetch(wanted, item_table, 0, ahead, 4)
    fetched_two = fetch(wanted, item_table, ahead, behind, 8)
    returned_one = exchange(fetched_one.reshape(owner_count, ahead, 1, dim)).reshape(-1, dim)
    returned_two = exchange(fetched_two.reshape(owner_count, behind, 1, dim)).reshape(-1, dim)
    slots_one = slot_users[:, :ahead].reshape(1, owner_count * ahead)
    slots_two = slot_users[:, ahead:capacity].reshape(1, owner_count * behind)
    hidden = jnp.dot(dense_input, w_bottom, preferred_element_type=jnp.float32)
    dense_out = jax.nn.silu(hidden)
    lens = jnp.broadcast_to(lengths[:, None].astype(jnp.float32), (user_count, dim))
    start = pool_first(slots_one, returned_one, user_count, 2)
    return pool_last(slots_two, returned_two, start, lens, dense_out, 5)


def solution(mesh):
    in_specs = (
        P(("row", "col"), None),
        P(("row", "col"), None),
        P(("row", "col"), None),
        P(("row", "col")),
        P(("row", "col"), None),
        P(),
    )
    out_specs = P(("row", "col"), None)
    return jax.shard_map(
        per_device, mesh=mesh, in_specs=in_specs, out_specs=out_specs, check_vma=False
    )
```

```python
import functools

import jax
import jax.numpy as jnp
from jax import lax
from jax.experimental import pallas as pl
from jax.experimental.pallas import tpu as pltpu
from jax.sharding import PartitionSpec as P

SLOT_PAD = 80
LANES = 128
FIRST_SLOTS = 20
PIECE = 1280


def round_up(value, unit):
    return (value + unit - 1) // unit * unit


def exchange(buffer):
    return lax.all_to_all(buffer, ("row", "col"), split_axis=0, concat_axis=0, tiled=True)


def route_kernel(me_ref, owner_ref, row_ref, len_ref, rows_out, users_out, assign_ref, value_ref):
    hist_len, user_count = owner_ref.shape
    owner_count = rows_out.shape[0]
    span = 2 * user_count
    lens = jnp.concatenate([len_ref[...], len_ref[...]], axis=1)
    owner_iota = lax.broadcasted_iota(jnp.int32, (owner_count, span), 0)
    slot_iota = lax.broadcasted_iota(jnp.int32, (SLOT_PAD, span), 0)
    place_iota = lax.broadcasted_iota(jnp.int32, (1, span), 1)
    second = (place_iota >= user_count).astype(jnp.int32)
    name = (place_iota - second * user_count + 1).astype(jnp.float32)
    earlier = lax.broadcasted_iota(jnp.int32, (span, span), 0)
    later = lax.broadcasted_iota(jnp.int32, (span, span), 1)
    counter = jnp.where(earlier < later, 1.0, 0.0).astype(jnp.bfloat16)
    offset = jnp.zeros((owner_count, 1), jnp.float32)
    for h in range(0, hist_len, 2):
        lanes = slice(h * user_count, h * user_count + span)
        pair = jnp.concatenate([owner_ref[h : h + 1, :], owner_ref[h + 1 : h + 2, :]], axis=1)
        owners = jnp.where(h + second < lens, pair, -1)
        hits = owners == owner_iota
        assign = jnp.where(hits, 1.0, 0.0)
        assign_ref[:, lanes] = assign.astype(jnp.bfloat16)
        counts = jnp.dot(assign_ref[:, lanes], counter, preferred_element_type=jnp.float32)
        rank = jnp.sum(jnp.where(hits, counts + offset, 0.0), axis=0, keepdims=True).astype(jnp.int32)
        offset = offset + counts[:, span - 1 :] + assign[:, span - 1 :]
        spot = rank == slot_iota
        rows = jnp.concatenate([row_ref[h : h + 1, :], row_ref[h + 1 : h + 2, :]], axis=1)
        high = (rows >> 8).astype(jnp.float32)
        low = (rows & 255).astype(jnp.float32)
        for part, content in enumerate((high, low, name)):
            value_ref[part * SLOT_PAD : (part + 1) * SLOT_PAD, lanes] = jnp.where(
                spot, content, 0.0
            ).astype(jnp.bfloat16)
    packed = lax.dot_general(
        assign_ref[...], value_ref[...], (((1,), (1,)), ((), ())), preferred_element_type=jnp.float32
    )
    names = packed[:, 2 * SLOT_PAD :]
    spare = me_ref[0, 0] * SLOT_PAD + lax.broadcasted_iota(jnp.int32, names.shape, 1)
    table_rows = (packed[:, :SLOT_PAD] * 256.0 + packed[:, SLOT_PAD : 2 * SLOT_PAD]).astype(jnp.int32)
    table_rows = jnp.where(names > 0.0, table_rows, spare)
    fill = jnp.zeros((owner_count, LANES - SLOT_PAD), jnp.int32)
    rows_out[...] = jnp.concatenate([table_rows, fill], axis=1)
    users_out[...] = jnp.concatenate([names.astype(jnp.int32), fill], axis=1)


def route(me, owner_t, row_t, lengths, owner_count):
    hist_len, user_count = owner_t.shape
    pos_count = hist_len * user_count
    shape = jax.ShapeDtypeStruct((owner_count, LANES), jnp.int32)
    return pl.pallas_call(
        route_kernel,
        in_specs=[
            pl.BlockSpec(memory_space=pltpu.SMEM),
            pl.BlockSpec(memory_space=pltpu.VMEM),
            pl.BlockSpec(memory_space=pltpu.VMEM),
            pl.BlockSpec(memory_space=pltpu.VMEM),
        ],
        out_shape=(shape, shape),
        scratch_shapes=[
            pltpu.VMEM((owner_count, pos_count), jnp.bfloat16),
            pltpu.VMEM((3 * SLOT_PAD, pos_count), jnp.bfloat16),
        ],
        name="route",
    )(jnp.full((1, 1), me, jnp.int32), owner_t, row_t, lengths.reshape(1, user_count))


def fetch_kernel(first, count, groups, wanted_ref, table_ref, out_ref, rows_ref, stage_ref, row_sems, in_sems, out_sems):
    sources = wanted_ref.shape[0]
    per_group = sources // groups
    span = per_group * count

    def learn(group):
        place = pl.ds(group * per_group, per_group)
        return pltpu.make_async_copy(wanted_ref.at[place], rows_ref.at[place], row_sems.at[group])

    def issue(group):
        def one_source(index, carry):
            source = group * per_group + index
            for c in range(count):
                pltpu.make_async_copy(
                    table_ref.at[pl.ds(rows_ref[source, 0, first + c], 1), :],
                    stage_ref.at[pl.ds(source * count + c, 1), :],
                    in_sems.at[group],
                ).start(priority=c % 2)
            return carry

        lax.fori_loop(0, per_group, one_source, 0)

    def store(group):
        place = pl.ds(group * span, span)
        return pltpu.make_async_copy(stage_ref.at[place, :], out_ref.at[place, :], out_sems.at[group])

    def arrive(group):
        place = pl.ds(group * span, span)
        pltpu.make_async_copy(table_ref.at[pl.ds(0, span), :], stage_ref.at[place, :], in_sems.at[group]).wait()
        store(group).start()

    for group in range(groups):
        learn(group).start()
    for group in range(groups):
        learn(group).wait()
        issue(group)
        if group > 0:
            arrive(group - 1)
    arrive(groups - 1)
    for group in range(groups):
        store(group).wait()


def fetch(wanted, item_table, first, count, groups):
    sources = wanted.shape[0]
    dim = item_table.shape[1]
    return pl.pallas_call(
        functools.partial(fetch_kernel, first, count, groups),
        in_specs=[pl.BlockSpec(memory_space=pltpu.HBM), pl.BlockSpec(memory_space=pltpu.HBM)],
        out_specs=pl.BlockSpec(memory_space=pltpu.HBM),
        out_shape=jax.ShapeDtypeStruct((sources * count, dim), jnp.float32),
        scratch_shapes=[
            pltpu.SMEM(wanted.shape, jnp.int32),
            pltpu.VMEM((sources * count, dim), jnp.float32),
            pltpu.SemaphoreType.DMA((groups,)),
            pltpu.SemaphoreType.DMA((groups,)),
            pltpu.SemaphoreType.DMA((groups,)),
        ],
        cost_estimate=pl.CostEstimate(
            flops=sources * count * 4000, bytes_accessed=sources * count * dim * 8, transcendentals=0
        ),
        compiler_params=pltpu.CompilerParams(vmem_limit_bytes=63 * 2**20),
        name="fetch",
    )(wanted, item_table)


def sum_rows(slot_ref, rows_ref, stage_ref, sems, before):
    user_count = before.shape[0]
    count = rows_ref.shape[0]
    starts = list(range(0, count, PIECE))
    copies = []
    for part, start in enumerate(starts):
        place = pl.ds(start, min(PIECE, count - start))
        copies.append(pltpu.make_async_copy(rows_ref.at[place, :], stage_ref.at[place, :], sems.at[part]))
        copies[-1].start()
    total = before
    for start, copy in zip(starts, copies):
        length = min(PIECE, count - start)
        users = lax.broadcasted_iota(jnp.int32, (user_count, length), 0) + 1
        selector = jnp.where(slot_ref[:, start : start + length] == users, 1.0, 0.0).astype(jnp.bfloat16)
        copy.wait()
        rows = stage_ref[start : start + length, :]
        high = rows.astype(jnp.bfloat16)
        low = (rows - high.astype(jnp.float32)).astype(jnp.bfloat16)
        total = total + jnp.dot(
            selector, jnp.concatenate([high, low], axis=1), preferred_element_type=jnp.float32
        )
    return total


def pool_first_kernel(slot_ref, rows_ref, total_ref, stage_ref, sems):
    total_ref[...] = sum_rows(slot_ref, rows_ref, stage_ref, sems, jnp.zeros(total_ref.shape, jnp.float32))


def pool_last_kernel(slot_ref, rows_ref, start_ref, len_ref, dense_ref, out_ref, stage_ref, sems):
    dim = rows_ref.shape[1]
    user_count = out_ref.shape[0]
    total = sum_rows(slot_ref, rows_ref, stage_ref, sems, start_ref[...])
    here = lax.broadcasted_iota(jnp.int32, (user_count, user_count), 0)
    there = lax.broadcasted_iota(jnp.int32, (user_count, user_count), 1)
    spread = jnp.where(here == there, len_ref[...].astype(jnp.float32), 0.0)
    lens = jnp.sum(spread, axis=1, keepdims=True)
    out_ref[:, :dim] = (total[:, :dim] + total[:, dim:]) / lens
    out_ref[:, dim:] = dense_ref[...]


def pool_scratch(count, dim):
    return [pltpu.VMEM((count, dim), jnp.float32), pltpu.SemaphoreType.DMA((pl.cdiv(count, PIECE),))]


def pool_first(slots, rows, user_count):
    count, dim = rows.shape
    return pl.pallas_call(
        pool_first_kernel,
        in_specs=[pl.BlockSpec(memory_space=pltpu.VMEM), pl.BlockSpec(memory_space=pltpu.HBM)],
        out_shape=jax.ShapeDtypeStruct((user_count, 2 * dim), jnp.float32),
        scratch_shapes=pool_scratch(count, dim),
        cost_estimate=pl.CostEstimate(flops=count * 4000, bytes_accessed=count * dim * 4, transcendentals=0),
        name="pool_first",
    )(slots, rows)


def pool_last(slots, rows, start, lengths, dense_out):
    count, dim = rows.shape
    user_count, dense_dim = dense_out.shape
    vmem = pl.BlockSpec(memory_space=pltpu.VMEM)
    return pl.pallas_call(
        pool_last_kernel,
        in_specs=[vmem, pl.BlockSpec(memory_space=pltpu.HBM), vmem, vmem, vmem],
        out_shape=jax.ShapeDtypeStruct((user_count, dim + dense_dim), jnp.float32),
        scratch_shapes=pool_scratch(count, dim),
        name="pool_last",
    )(slots, rows, start, lengths.reshape(1, user_count), dense_out)


def per_device(item_table, owner_ids, row_ids, lengths, dense_input, w_bottom):
    user_count, hist_len = owner_ids.shape
    dim = item_table.shape[1]
    owner_count = lax.axis_size("row") * lax.axis_size("col")
    capacity = 3 * user_count * hist_len // (2 * owner_count)
    ahead = FIRST_SLOTS
    behind = capacity - ahead
    me = lax.axis_index("row") * lax.axis_size("col") + lax.axis_index("col")
    table_rows, slot_users = route(me, owner_ids.T, row_ids.T, lengths, owner_count)
    wanted = exchange(table_rows.reshape(owner_count, 1, LANES))
    fetched_one = fetch(wanted, item_table, 0, ahead, 8)
    fetched_two = fetch(wanted, item_table, ahead, behind, 8)
    returned_one = exchange(fetched_one.reshape(owner_count, ahead, 1, dim)).reshape(-1, dim)
    returned_two = exchange(fetched_two.reshape(owner_count, behind, 1, dim)).reshape(-1, dim)
    slots_one = slot_users[:, :ahead].reshape(1, owner_count * ahead)
    slots_two = slot_users[:, ahead:capacity].reshape(1, owner_count * behind)
    hidden = jnp.dot(dense_input, w_bottom, preferred_element_type=jnp.float32)
    dense_out = jax.nn.silu(hidden)
    start = pool_first(slots_one, returned_one, user_count)
    return pool_last(slots_two, returned_two, start, lengths, dense_out)


def solution(mesh):
    in_specs = (
        P(("row", "col"), None),
        P(("row", "col"), None),
        P(("row", "col"), None),
        P(("row", "col")),
        P(("row", "col"), None),
        P(),
    )
    out_specs = P(("row", "col"), None)
    return jax.shard_map(
        per_device, mesh=mesh, in_specs=in_specs, out_specs=out_specs, check_vma=False
    )
```

```python
import functools

import jax
import jax.numpy as jnp
from jax import lax
from jax.experimental import pallas as pl
from jax.experimental.pallas import tpu as pltpu
from jax.sharding import PartitionSpec as P

SLOT_PAD = 80
LANES = 128
PIECE = 1280
VMEM_LIMIT = 60 * 2**20


def round_up(value, unit):
    return (value + unit - 1) // unit * unit


def exchange(buffer):
    return lax.all_to_all(buffer, ("row", "col"), split_axis=0, concat_axis=0, tiled=True)


def route_kernel(me_ref, owner_ref, row_ref, len_ref, rows_out, users_out, assign_ref, value_ref):
    hist_len, user_count = owner_ref.shape
    owner_count = rows_out.shape[0]
    span = 2 * user_count
    lens = jnp.concatenate([len_ref[...], len_ref[...]], axis=1)
    owner_iota = lax.broadcasted_iota(jnp.int32, (owner_count, span), 0)
    slot_iota = lax.broadcasted_iota(jnp.int32, (SLOT_PAD, span), 0)
    place_iota = lax.broadcasted_iota(jnp.int32, (1, span), 1)
    second = (place_iota >= user_count).astype(jnp.int32)
    name = (place_iota - second * user_count + 1).astype(jnp.float32)
    earlier = lax.broadcasted_iota(jnp.int32, (span, span), 0)
    later = lax.broadcasted_iota(jnp.int32, (span, span), 1)
    counter = jnp.where(earlier < later, 1.0, 0.0).astype(jnp.bfloat16)
    offset = jnp.zeros((owner_count, 1), jnp.float32)
    for h in range(0, hist_len, 2):
        lanes = slice(h * user_count, h * user_count + span)
        pair = jnp.concatenate([owner_ref[h : h + 1, :], owner_ref[h + 1 : h + 2, :]], axis=1)
        owners = jnp.where(h + second < lens, pair, -1)
        hits = owners == owner_iota
        assign = jnp.where(hits, 1.0, 0.0)
        assign_ref[:, lanes] = assign.astype(jnp.bfloat16)
        counts = jnp.dot(assign_ref[:, lanes], counter, preferred_element_type=jnp.float32)
        rank = jnp.sum(jnp.where(hits, counts + offset, 0.0), axis=0, keepdims=True).astype(jnp.int32)
        offset = offset + counts[:, span - 1 :] + assign[:, span - 1 :]
        spot = rank == slot_iota
        rows = jnp.concatenate([row_ref[h : h + 1, :], row_ref[h + 1 : h + 2, :]], axis=1)
        high = (rows >> 8).astype(jnp.float32)
        low = (rows & 255).astype(jnp.float32)
        for part, content in enumerate((high, low, name)):
            value_ref[part * SLOT_PAD : (part + 1) * SLOT_PAD, lanes] = jnp.where(
                spot, content, 0.0
            ).astype(jnp.bfloat16)
    packed = lax.dot_general(
        assign_ref[...], value_ref[...], (((1,), (1,)), ((), ())), preferred_element_type=jnp.float32
    )
    names = packed[:, 2 * SLOT_PAD :]
    spare = me_ref[0, 0] * SLOT_PAD + lax.broadcasted_iota(jnp.int32, names.shape, 1)
    table_rows = (packed[:, :SLOT_PAD] * 256.0 + packed[:, SLOT_PAD : 2 * SLOT_PAD]).astype(jnp.int32)
    table_rows = jnp.where(names > 0.0, table_rows, spare)
    fill = jnp.zeros((owner_count, LANES - SLOT_PAD), jnp.int32)
    rows_out[...] = jnp.concatenate([table_rows, fill], axis=1)
    users_out[...] = jnp.concatenate([names.astype(jnp.int32), fill], axis=1)


def route(me, owner_t, row_t, lengths, owner_count):
    hist_len, user_count = owner_t.shape
    pos_count = hist_len * user_count
    shape = jax.ShapeDtypeStruct((owner_count, LANES), jnp.int32)
    return pl.pallas_call(
        route_kernel,
        in_specs=[
            pl.BlockSpec(memory_space=pltpu.SMEM),
            pl.BlockSpec(memory_space=pltpu.VMEM),
            pl.BlockSpec(memory_space=pltpu.VMEM),
            pl.BlockSpec(memory_space=pltpu.VMEM),
        ],
        out_shape=(shape, shape),
        scratch_shapes=[
            pltpu.VMEM((owner_count, pos_count), jnp.bfloat16),
            pltpu.VMEM((3 * SLOT_PAD, pos_count), jnp.bfloat16),
        ],
        compiler_params=pltpu.CompilerParams(vmem_limit_bytes=VMEM_LIMIT),
        name="route",
    )(jnp.full((1, 1), me, jnp.int32), owner_t, row_t, lengths.reshape(1, user_count))


def fetch_kernel(count, groups, wanted_ref, table_ref, out_ref, rows_ref, near_ref, stage_ref, row_sems, table_sems, out_sems):
    part = table_ref.shape[0] // groups
    sources = wanted_ref.shape[0]
    per_group = sources // groups
    span = per_group * count

    def learn(group):
        place = pl.ds(group * per_group, per_group)
        return pltpu.make_async_copy(wanted_ref.at[place], rows_ref.at[place], row_sems.at[group])

    def store(group):
        place = pl.ds(group * span, span)
        return pltpu.make_async_copy(stage_ref.at[place], out_ref.at[place], out_sems.at[group])

    def approach(group):
        place = pl.ds(group * part, part)
        return pltpu.make_async_copy(table_ref.at[place], near_ref.at[place], table_sems.at[group])

    for group in range(groups):
        approach(group).start(priority=group % 2)
    for group in range(groups):
        learn(group).start()
    for group in range(groups):
        learn(group).wait()
    for group in range(groups):
        approach(group).wait()
    for group in range(groups):

        def one_source(index, carry):
            source = group * per_group + index
            for c in range(count):
                stage_ref[pl.ds(source * count + c, 1)] = near_ref[pl.ds(rows_ref[source, 0, c], 1)]
            return carry

        lax.fori_loop(0, per_group, one_source, 0)
        store(group).start()
    for group in range(groups):
        store(group).wait()


def fetch(wanted, table, count, groups):
    sources = wanted.shape[0]
    shape = (sources * count,) + table.shape[1:]
    return pl.pallas_call(
        functools.partial(fetch_kernel, count, groups),
        in_specs=[pl.BlockSpec(memory_space=pl.ANY), pl.BlockSpec(memory_space=pl.ANY)],
        out_specs=pl.BlockSpec(memory_space=pl.ANY),
        out_shape=jax.ShapeDtypeStruct(shape, jnp.float32),
        scratch_shapes=[
            pltpu.SMEM(wanted.shape, jnp.int32),
            pltpu.VMEM(table.shape, jnp.float32),
            pltpu.VMEM(shape, jnp.float32),
            pltpu.SemaphoreType.DMA((groups,)),
            pltpu.SemaphoreType.DMA((groups,)),
            pltpu.SemaphoreType.DMA((groups,)),
        ],
        compiler_params=pltpu.CompilerParams(vmem_limit_bytes=VMEM_LIMIT),
        name="fetch",
    )(wanted, table)


def sum_rows(slot_ref, rows_ref, stage_ref, sems, before):
    user_count = before.shape[0]
    count = rows_ref.shape[0]
    starts = list(range(0, count, PIECE))
    copies = []
    for part, start in enumerate(starts):
        place = pl.ds(start, min(PIECE, count - start))
        copies.append(pltpu.make_async_copy(rows_ref.at[place, :], stage_ref.at[place, :], sems.at[part]))
        copies[-1].start()
    total = before
    for start, copy in zip(starts, copies):
        length = min(PIECE, count - start)
        users = lax.broadcasted_iota(jnp.int32, (user_count, length), 0) + 1
        selector = jnp.where(slot_ref[:, start : start + length] == users, 1.0, 0.0).astype(jnp.bfloat16)
        copy.wait()
        rows = stage_ref[start : start + length, :]
        high = rows.astype(jnp.bfloat16)
        low = (rows - high.astype(jnp.float32)).astype(jnp.bfloat16)
        total = total + jnp.dot(
            selector, jnp.concatenate([high, low], axis=1), preferred_element_type=jnp.float32
        )
    return total


def pool_kernel(slot_ref, rows_ref, len_ref, dense_ref, out_ref, stage_ref, sems):
    dim = rows_ref.shape[1]
    user_count = out_ref.shape[0]
    total = sum_rows(slot_ref, rows_ref, stage_ref, sems, jnp.zeros((user_count, 2 * dim), jnp.float32))
    here = lax.broadcasted_iota(jnp.int32, (user_count, user_count), 0)
    there = lax.broadcasted_iota(jnp.int32, (user_count, user_count), 1)
    spread = jnp.where(here == there, len_ref[...].astype(jnp.float32), 0.0)
    lens = jnp.sum(spread, axis=1, keepdims=True)
    out_ref[:, :dim] = (total[:, :dim] + total[:, dim:]) / lens
    out_ref[:, dim:] = dense_ref[...]


def pool_scratch(count, dim):
    return [pltpu.VMEM((count, dim), jnp.float32), pltpu.SemaphoreType.DMA((pl.cdiv(count, PIECE),))]


def pool(slots, rows, lengths, dense_out):
    count, dim = rows.shape
    user_count, dense_dim = dense_out.shape
    vmem = pl.BlockSpec(memory_space=pltpu.VMEM)
    return pl.pallas_call(
        pool_kernel,
        in_specs=[vmem, pl.BlockSpec(memory_space=pl.ANY), vmem, vmem],
        out_shape=jax.ShapeDtypeStruct((user_count, dim + dense_dim), jnp.float32),
        scratch_shapes=pool_scratch(count, dim),
        compiler_params=pltpu.CompilerParams(vmem_limit_bytes=VMEM_LIMIT),
        name="pool",
    )(slots, rows, lengths.reshape(1, user_count), dense_out)


def per_device(item_table, owner_ids, row_ids, lengths, dense_input, w_bottom):
    user_count, hist_len = owner_ids.shape
    dim = item_table.shape[1]
    owner_count = lax.axis_size("row") * lax.axis_size("col")
    capacity = 3 * user_count * hist_len // (2 * owner_count)
    slot_total = owner_count * capacity
    me = lax.axis_index("row") * lax.axis_size("col") + lax.axis_index("col")
    table_rows, slot_users = route(me, owner_ids.T, row_ids.T, lengths, owner_count)
    wanted = exchange(table_rows.reshape(owner_count, 1, LANES))
    fetched = fetch(wanted, item_table.reshape(-1, 1, dim), capacity, 8)
    returned = exchange(fetched.reshape(owner_count, capacity, 1, dim)).reshape(slot_total, dim)
    slots = slot_users[:, :capacity].reshape(1, slot_total)
    hidden = jnp.dot(dense_input, w_bottom, preferred_element_type=jnp.float32)
    dense_out = jax.nn.silu(hidden)
    return pool(slots, returned, lengths, dense_out)


def solution(mesh):
    in_specs = (
        P(("row", "col"), None),
        P(("row", "col"), None),
        P(("row", "col"), None),
        P(("row", "col")),
        P(("row", "col"), None),
        P(),
    )
    out_specs = P(("row", "col"), None)
    return jax.shard_map(
        per_device, mesh=mesh, in_specs=in_specs, out_specs=out_specs, check_vma=False
    )
```

```python
import functools

import jax
import jax.numpy as jnp
from jax import lax
from jax.experimental import pallas as pl
from jax.experimental.pallas import tpu as pltpu
from jax.sharding import PartitionSpec as P

SLOT_PAD = 80
LANES = 128
PIECE = 1280
TABLE_PIECES = 8
VMEM_LIMIT = 60 * 2**20


def round_up(value, unit):
    return (value + unit - 1) // unit * unit


def exchange(buffer):
    return lax.all_to_all(buffer, ("row", "col"), split_axis=0, concat_axis=0, tiled=True)


def route_kernel(me_ref, owner_ref, row_ref, len_ref, rows_out, users_out, assign_ref, value_ref):
    hist_len, user_count = owner_ref.shape
    owner_count = rows_out.shape[0]
    span = 2 * user_count
    lens = jnp.concatenate([len_ref[...], len_ref[...]], axis=1)
    owner_iota = lax.broadcasted_iota(jnp.int32, (owner_count, span), 0)
    slot_iota = lax.broadcasted_iota(jnp.int32, (SLOT_PAD, span), 0)
    place_iota = lax.broadcasted_iota(jnp.int32, (1, span), 1)
    second = (place_iota >= user_count).astype(jnp.int32)
    name = (place_iota - second * user_count + 1).astype(jnp.float32)
    earlier = lax.broadcasted_iota(jnp.int32, (span, span), 0)
    later = lax.broadcasted_iota(jnp.int32, (span, span), 1)
    counter = jnp.where(earlier < later, 1.0, 0.0).astype(jnp.bfloat16)
    offset = jnp.zeros((owner_count, 1), jnp.float32)
    for h in range(0, hist_len, 2):
        lanes = slice(h * user_count, h * user_count + span)
        pair = jnp.concatenate([owner_ref[h : h + 1, :], owner_ref[h + 1 : h + 2, :]], axis=1)
        owners = jnp.where(h + second < lens, pair, -1)
        hits = owners == owner_iota
        assign = jnp.where(hits, 1.0, 0.0)
        assign_ref[:, lanes] = assign.astype(jnp.bfloat16)
        counts = jnp.dot(assign_ref[:, lanes], counter, preferred_element_type=jnp.float32)
        rank = jnp.sum(jnp.where(hits, counts + offset, 0.0), axis=0, keepdims=True).astype(jnp.int32)
        offset = offset + counts[:, span - 1 :] + assign[:, span - 1 :]
        spot = rank == slot_iota
        rows = jnp.concatenate([row_ref[h : h + 1, :], row_ref[h + 1 : h + 2, :]], axis=1)
        high = (rows >> 8).astype(jnp.float32)
        low = (rows & 255).astype(jnp.float32)
        for part, content in enumerate((high, low, name)):
            value_ref[part * SLOT_PAD : (part + 1) * SLOT_PAD, lanes] = jnp.where(
                spot, content, 0.0
            ).astype(jnp.bfloat16)
    packed = lax.dot_general(
        assign_ref[...], value_ref[...], (((1,), (1,)), ((), ())), preferred_element_type=jnp.float32
    )
    names = packed[:, 2 * SLOT_PAD :]
    spare = me_ref[0, 0] * SLOT_PAD + lax.broadcasted_iota(jnp.int32, names.shape, 1)
    table_rows = (packed[:, :SLOT_PAD] * 256.0 + packed[:, SLOT_PAD : 2 * SLOT_PAD]).astype(jnp.int32)
    table_rows = jnp.where(names > 0.0, table_rows, spare)
    fill = jnp.zeros((owner_count, LANES - SLOT_PAD), jnp.int32)
    rows_out[...] = jnp.concatenate([table_rows, fill], axis=1)
    users_out[...] = jnp.concatenate([names.astype(jnp.int32), fill], axis=1)


def route(me, owner_t, row_t, lengths, owner_count):
    hist_len, user_count = owner_t.shape
    pos_count = hist_len * user_count
    shape = jax.ShapeDtypeStruct((owner_count, LANES), jnp.int32)
    return pl.pallas_call(
        route_kernel,
        in_specs=[
            pl.BlockSpec(memory_space=pltpu.SMEM),
            pl.BlockSpec(memory_space=pltpu.VMEM),
            pl.BlockSpec(memory_space=pltpu.VMEM),
            pl.BlockSpec(memory_space=pltpu.VMEM),
        ],
        out_shape=(shape, shape),
        scratch_shapes=[
            pltpu.VMEM((owner_count, pos_count), jnp.bfloat16),
            pltpu.VMEM((3 * SLOT_PAD, pos_count), jnp.bfloat16),
        ],
        compiler_params=pltpu.CompilerParams(vmem_limit_bytes=VMEM_LIMIT),
        name="route",
    )(jnp.full((1, 1), me, jnp.int32), owner_t, row_t, lengths.reshape(1, user_count))


def fetch_kernel(count, groups, wanted_ref, table_ref, out_ref, rows_ref, near_ref, stage_ref, row_sems, table_sems, out_sems):
    part = table_ref.shape[0] // TABLE_PIECES
    sources = wanted_ref.shape[0]
    per_group = sources // groups
    span = per_group * count

    def learn(group):
        place = pl.ds(group * per_group, per_group)
        return pltpu.make_async_copy(wanted_ref.at[place], rows_ref.at[place], row_sems.at[group])

    def store(group):
        place = pl.ds(group * span, span)
        return pltpu.make_async_copy(stage_ref.at[place], out_ref.at[place], out_sems.at[group])

    def approach(group):
        place = pl.ds(group * part, part)
        return pltpu.make_async_copy(table_ref.at[place], near_ref.at[place], table_sems.at[group])

    for group in range(TABLE_PIECES):
        approach(group).start(priority=group % 2)
    for group in range(groups):
        learn(group).start()
    for group in range(groups):
        learn(group).wait()
    for group in range(TABLE_PIECES):
        approach(group).wait()
    for group in range(groups):

        for source in range(group * per_group, (group + 1) * per_group):
            for c in range(count):
                stage_ref[source * count + c] = near_ref[rows_ref[source, 0, c]]
        store(group).start()
    for group in range(groups):
        store(group).wait()


def fetch(wanted, table, count, groups):
    sources = wanted.shape[0]
    shape = (sources * count,) + table.shape[1:]
    return pl.pallas_call(
        functools.partial(fetch_kernel, count, groups),
        in_specs=[pl.BlockSpec(memory_space=pl.ANY), pl.BlockSpec(memory_space=pl.ANY)],
        out_specs=pl.BlockSpec(memory_space=pl.ANY),
        out_shape=jax.ShapeDtypeStruct(shape, jnp.float32),
        scratch_shapes=[
            pltpu.SMEM(wanted.shape, jnp.int32),
            pltpu.VMEM(table.shape, jnp.float32),
            pltpu.VMEM(shape, jnp.float32),
            pltpu.SemaphoreType.DMA((groups,)),
            pltpu.SemaphoreType.DMA((TABLE_PIECES,)),
            pltpu.SemaphoreType.DMA((groups,)),
        ],
        compiler_params=pltpu.CompilerParams(vmem_limit_bytes=VMEM_LIMIT),
        name="fetch",
    )(wanted, table)


def sum_rows(slot_ref, rows_ref, stage_ref, sems, before):
    user_count = before.shape[0]
    count = rows_ref.shape[0]
    starts = list(range(0, count, PIECE))
    copies = []
    for part, start in enumerate(starts):
        place = pl.ds(start, min(PIECE, count - start))
        copies.append(pltpu.make_async_copy(rows_ref.at[place, :], stage_ref.at[place, :], sems.at[part]))
        copies[-1].start()
    total = before
    for start, copy in zip(starts, copies):
        length = min(PIECE, count - start)
        users = lax.broadcasted_iota(jnp.int32, (user_count, length), 0) + 1
        selector = jnp.where(slot_ref[:, start : start + length] == users, 1.0, 0.0).astype(jnp.bfloat16)
        copy.wait()
        rows = stage_ref[start : start + length, :]
        high = rows.astype(jnp.bfloat16)
        low = (rows - high.astype(jnp.float32)).astype(jnp.bfloat16)
        total = total + jnp.dot(
            selector, jnp.concatenate([high, low], axis=1), preferred_element_type=jnp.float32
        )
    return total


def pool_kernel(slot_ref, rows_ref, len_ref, dense_ref, out_ref, stage_ref, sems):
    dim = rows_ref.shape[1]
    user_count = out_ref.shape[0]
    total = sum_rows(slot_ref, rows_ref, stage_ref, sems, jnp.zeros((user_count, 2 * dim), jnp.float32))
    here = lax.broadcasted_iota(jnp.int32, (user_count, user_count), 0)
    there = lax.broadcasted_iota(jnp.int32, (user_count, user_count), 1)
    spread = jnp.where(here == there, len_ref[...].astype(jnp.float32), 0.0)
    lens = jnp.sum(spread, axis=1, keepdims=True)
    out_ref[:, :dim] = (total[:, :dim] + total[:, dim:]) / lens
    out_ref[:, dim:] = dense_ref[...]


def pool_scratch(count, dim):
    return [pltpu.VMEM((count, dim), jnp.float32), pltpu.SemaphoreType.DMA((pl.cdiv(count, PIECE),))]


def pool(slots, rows, lengths, dense_out):
    count, dim = rows.shape
    user_count, dense_dim = dense_out.shape
    vmem = pl.BlockSpec(memory_space=pltpu.VMEM)
    return pl.pallas_call(
        pool_kernel,
        in_specs=[vmem, pl.BlockSpec(memory_space=pl.ANY), vmem, vmem],
        out_shape=jax.ShapeDtypeStruct((user_count, dim + dense_dim), jnp.float32),
        scratch_shapes=pool_scratch(count, dim),
        compiler_params=pltpu.CompilerParams(vmem_limit_bytes=VMEM_LIMIT),
        name="pool",
    )(slots, rows, lengths.reshape(1, user_count), dense_out)


def per_device(item_table, owner_ids, row_ids, lengths, dense_input, w_bottom):
    user_count, hist_len = owner_ids.shape
    dim = item_table.shape[1]
    owner_count = lax.axis_size("row") * lax.axis_size("col")
    capacity = 3 * user_count * hist_len // (2 * owner_count)
    slot_total = owner_count * capacity
    me = lax.axis_index("row") * lax.axis_size("col") + lax.axis_index("col")
    table_rows, slot_users = route(me, owner_ids.T, row_ids.T, lengths, owner_count)
    wanted = exchange(table_rows.reshape(owner_count, 1, LANES))
    fetched = fetch(wanted, item_table.reshape(-1, 1, dim), capacity, 8)
    returned = exchange(fetched.reshape(owner_count, capacity, 1, dim)).reshape(slot_total, dim)
    slots = slot_users[:, :capacity].reshape(1, slot_total)
    hidden = jnp.dot(dense_input, w_bottom, preferred_element_type=jnp.float32)
    dense_out = jax.nn.silu(hidden)
    return pool(slots, returned, lengths, dense_out)


def solution(mesh):
    in_specs = (
        P(("row", "col"), None),
        P(("row", "col"), None),
        P(("row", "col"), None),
        P(("row", "col")),
        P(("row", "col"), None),
        P(),
    )
    out_specs = P(("row", "col"), None)
    return jax.shard_map(
        per_device, mesh=mesh, in_specs=in_specs, out_specs=out_specs, check_vma=False
    )
```

```python
import functools

import jax
import jax.numpy as jnp
from jax import lax
from jax.experimental import pallas as pl
from jax.experimental.pallas import tpu as pltpu
from jax.sharding import PartitionSpec as P

SLOT_PAD = 80
LANES = 128
PIECE = 1280
TABLE_PIECES = 8
VMEM_LIMIT = 60 * 2**20


def round_up(value, unit):
    return (value + unit - 1) // unit * unit


def exchange(buffer):
    return lax.all_to_all(buffer, ("row", "col"), split_axis=0, concat_axis=0, tiled=True)


def route_kernel(me_ref, owner_ref, row_ref, len_ref, rows_out, users_out, assign_ref, value_ref):
    hist_len, user_count = owner_ref.shape
    owner_count = rows_out.shape[0]
    span = 2 * user_count
    lens = jnp.concatenate([len_ref[...], len_ref[...]], axis=1)
    owner_iota = lax.broadcasted_iota(jnp.int32, (owner_count, span), 0)
    slot_iota = lax.broadcasted_iota(jnp.int32, (SLOT_PAD, span), 0)
    place_iota = lax.broadcasted_iota(jnp.int32, (1, span), 1)
    second = (place_iota >= user_count).astype(jnp.int32)
    name = (place_iota - second * user_count + 1).astype(jnp.float32)
    earlier = lax.broadcasted_iota(jnp.int32, (span, span), 0)
    later = lax.broadcasted_iota(jnp.int32, (span, span), 1)
    counter = jnp.where(earlier < later, 1.0, 0.0).astype(jnp.bfloat16)
    offset = jnp.zeros((owner_count, 1), jnp.float32)
    for h in range(0, hist_len, 2):
        lanes = slice(h * user_count, h * user_count + span)
        pair = jnp.concatenate([owner_ref[h : h + 1, :], owner_ref[h + 1 : h + 2, :]], axis=1)
        owners = jnp.where(h + second < lens, pair, -1)
        hits = owners == owner_iota
        assign = jnp.where(hits, 1.0, 0.0)
        assign_ref[:, lanes] = assign.astype(jnp.bfloat16)
        counts = jnp.dot(assign_ref[:, lanes], counter, preferred_element_type=jnp.float32)
        rank = jnp.sum(jnp.where(hits, counts + offset, 0.0), axis=0, keepdims=True).astype(jnp.int32)
        offset = offset + counts[:, span - 1 :] + assign[:, span - 1 :]
        spot = rank == slot_iota
        rows = jnp.concatenate([row_ref[h : h + 1, :], row_ref[h + 1 : h + 2, :]], axis=1)
        high = (rows >> 8).astype(jnp.float32)
        low = (rows & 255).astype(jnp.float32)
        for part, content in enumerate((high, low, name)):
            value_ref[part * SLOT_PAD : (part + 1) * SLOT_PAD, lanes] = jnp.where(
                spot, content, 0.0
            ).astype(jnp.bfloat16)
    packed = lax.dot_general(
        assign_ref[...], value_ref[...], (((1,), (1,)), ((), ())), preferred_element_type=jnp.float32
    )
    names = packed[:, 2 * SLOT_PAD :]
    spare = me_ref[0, 0] * SLOT_PAD + lax.broadcasted_iota(jnp.int32, names.shape, 1)
    table_rows = (packed[:, :SLOT_PAD] * 256.0 + packed[:, SLOT_PAD : 2 * SLOT_PAD]).astype(jnp.int32)
    table_rows = jnp.where(names > 0.0, table_rows, spare)
    fill = jnp.zeros((owner_count, LANES - SLOT_PAD), jnp.int32)
    rows_out[...] = jnp.concatenate([table_rows, fill], axis=1)
    users_out[...] = jnp.concatenate([names.astype(jnp.int32), fill], axis=1)


def route(me, owner_t, row_t, lengths, owner_count):
    hist_len, user_count = owner_t.shape
    pos_count = hist_len * user_count
    shape = jax.ShapeDtypeStruct((owner_count, LANES), jnp.int32)
    return pl.pallas_call(
        route_kernel,
        in_specs=[
            pl.BlockSpec(memory_space=pltpu.SMEM),
            pl.BlockSpec(memory_space=pltpu.VMEM),
            pl.BlockSpec(memory_space=pltpu.VMEM),
            pl.BlockSpec(memory_space=pltpu.VMEM),
        ],
        out_shape=(shape, shape),
        scratch_shapes=[
            pltpu.VMEM((owner_count, pos_count), jnp.bfloat16),
            pltpu.VMEM((3 * SLOT_PAD, pos_count), jnp.bfloat16),
        ],
        compiler_params=pltpu.CompilerParams(vmem_limit_bytes=VMEM_LIMIT),
        name="route",
    )(jnp.full((1, 1), me, jnp.int32), owner_t, row_t, lengths.reshape(1, user_count))


def fetch_kernel(count, groups, wanted_ref, table_ref, out_ref, rows_ref, near_ref, stage_ref, row_sems, table_sems, out_sems):
    part = table_ref.shape[0] // TABLE_PIECES
    sources = wanted_ref.shape[0]
    per_group = sources // groups
    span = per_group * count

    def learn(group):
        place = pl.ds(group * per_group, per_group)
        return pltpu.make_async_copy(wanted_ref.at[place], rows_ref.at[place], row_sems.at[group])

    def store(group):
        place = pl.ds(group * span, span)
        return pltpu.make_async_copy(stage_ref.at[place], out_ref.at[place], out_sems.at[group])

    def approach(group):
        place = pl.ds(group * part, part)
        return pltpu.make_async_copy(table_ref.at[place], near_ref.at[place], table_sems.at[group])

    for group in range(TABLE_PIECES):
        approach(group).start(priority=group % 2)
    for group in range(groups):
        learn(group).start()
    for group in range(groups):
        learn(group).wait()
    for group in range(TABLE_PIECES):
        approach(group).wait()
    for group in range(groups):

        for source in range(group * per_group, (group + 1) * per_group):
            for c in range(count):
                stage_ref[source * count + c] = near_ref[rows_ref[source, 0, c]]
        if group > 0:
            store(group - 1).start()
    store(groups - 1).start()
    for group in range(groups):
        store(group).wait()


def fetch(wanted, table, count, groups):
    sources = wanted.shape[0]
    shape = (sources * count,) + table.shape[1:]
    return pl.pallas_call(
        functools.partial(fetch_kernel, count, groups),
        in_specs=[pl.BlockSpec(memory_space=pl.ANY), pl.BlockSpec(memory_space=pl.ANY)],
        out_specs=pl.BlockSpec(memory_space=pl.ANY),
        out_shape=jax.ShapeDtypeStruct(shape, jnp.float32),
        scratch_shapes=[
            pltpu.SMEM(wanted.shape, jnp.int32),
            pltpu.VMEM(table.shape, jnp.float32),
            pltpu.VMEM(shape, jnp.float32),
            pltpu.SemaphoreType.DMA((groups,)),
            pltpu.SemaphoreType.DMA((TABLE_PIECES,)),
            pltpu.SemaphoreType.DMA((groups,)),
        ],
        compiler_params=pltpu.CompilerParams(vmem_limit_bytes=VMEM_LIMIT),
        name="fetch",
    )(wanted, table)


def sum_rows(slot_ref, rows_ref, stage_ref, sems, before):
    user_count = before.shape[0]
    count = rows_ref.shape[0]
    starts = list(range(0, count, PIECE))
    copies = []
    for part, start in enumerate(starts):
        place = pl.ds(start, min(PIECE, count - start))
        copies.append(pltpu.make_async_copy(rows_ref.at[place, :], stage_ref.at[place, :], sems.at[part]))
        copies[-1].start()
    total = before
    for start, copy in zip(starts, copies):
        length = min(PIECE, count - start)
        users = lax.broadcasted_iota(jnp.int32, (user_count, length), 0) + 1
        selector = jnp.where(slot_ref[:, start : start + length] == users, 1.0, 0.0).astype(jnp.bfloat16)
        copy.wait()
        rows = stage_ref[start : start + length, :]
        high = rows.astype(jnp.bfloat16)
        low = (rows - high.astype(jnp.float32)).astype(jnp.bfloat16)
        total = total + jnp.dot(
            selector, jnp.concatenate([high, low], axis=1), preferred_element_type=jnp.float32
        )
    return total


def pool_kernel(slot_ref, rows_ref, len_ref, dense_ref, out_ref, stage_ref, sems):
    dim = rows_ref.shape[1]
    user_count = out_ref.shape[0]
    total = sum_rows(slot_ref, rows_ref, stage_ref, sems, jnp.zeros((user_count, 2 * dim), jnp.float32))
    here = lax.broadcasted_iota(jnp.int32, (user_count, user_count), 0)
    there = lax.broadcasted_iota(jnp.int32, (user_count, user_count), 1)
    spread = jnp.where(here == there, len_ref[...].astype(jnp.float32), 0.0)
    lens = jnp.sum(spread, axis=1, keepdims=True)
    out_ref[:, :dim] = (total[:, :dim] + total[:, dim:]) / lens
    out_ref[:, dim:] = dense_ref[...]


def pool_scratch(count, dim):
    return [pltpu.VMEM((count, dim), jnp.float32), pltpu.SemaphoreType.DMA((pl.cdiv(count, PIECE),))]


def pool(slots, rows, lengths, dense_out):
    count, dim = rows.shape
    user_count, dense_dim = dense_out.shape
    vmem = pl.BlockSpec(memory_space=pltpu.VMEM)
    return pl.pallas_call(
        pool_kernel,
        in_specs=[vmem, pl.BlockSpec(memory_space=pl.ANY), vmem, vmem],
        out_shape=jax.ShapeDtypeStruct((user_count, dim + dense_dim), jnp.float32),
        scratch_shapes=pool_scratch(count, dim),
        compiler_params=pltpu.CompilerParams(vmem_limit_bytes=VMEM_LIMIT),
        name="pool",
    )(slots, rows, lengths.reshape(1, user_count), dense_out)


def per_device(item_table, owner_ids, row_ids, lengths, dense_input, w_bottom):
    user_count, hist_len = owner_ids.shape
    dim = item_table.shape[1]
    owner_count = lax.axis_size("row") * lax.axis_size("col")
    capacity = 3 * user_count * hist_len // (2 * owner_count)
    slot_total = owner_count * capacity
    me = lax.axis_index("row") * lax.axis_size("col") + lax.axis_index("col")
    table_rows, slot_users = route(me, owner_ids.T, row_ids.T, lengths, owner_count)
    wanted = exchange(table_rows.reshape(owner_count, 1, LANES))
    fetched = fetch(wanted, item_table.reshape(-1, 1, dim), capacity, 16)
    returned = exchange(fetched.reshape(owner_count, capacity, 1, dim)).reshape(slot_total, dim)
    slots = slot_users[:, :capacity].reshape(1, slot_total)
    hidden = jnp.dot(dense_input, w_bottom, preferred_element_type=jnp.float32)
    dense_out = jax.nn.silu(hidden)
    return pool(slots, returned, lengths, dense_out)


def solution(mesh):
    in_specs = (
        P(("row", "col"), None),
        P(("row", "col"), None),
        P(("row", "col"), None),
        P(("row", "col")),
        P(("row", "col"), None),
        P(),
    )
    out_specs = P(("row", "col"), None)
    return jax.shard_map(
        per_device, mesh=mesh, in_specs=in_specs, out_specs=out_specs, check_vma=False
    )
```
